1024 devices in a mesh: group: 2 (over y_hi), row: 64 (over z, y_lo), col: 8 (over x, core).
Axes of the slice: x: 4, y: 4 (y_hi: 2, y_lo: 2; y = y_hi * 2 + y_lo), z: 32, core: 2. Of those that a mesh axis runs over, the one named last changes fastest.
Arguments:
- tokens: bfloat16 [4096, 5120], P('row', ('group', 'col')), may hold values from -6 to 6
- cotangent: bfloat16 [4096, 12800], P(('group', 'col'), 'row'), may hold values from -0.09375 to 0.09375
- master: float32 [12800, 5120], P('row', ('group', 'col')), may hold values from -0.078125 to 0.078125
- moment: float32 [12800, 5120], P('row', ('group', 'col')), may hold values from -6 to 6
- second: float32 [12800, 5120], P('row', ('group', 'col')), may hold values from 0.1 to 4
- prompts: bfloat16 [1024, 5120], P(('group', 'col')), may hold values from -6 to 6
- up_weight: bfloat16 [12800, 5120], P('row'), may hold values from -0.078125 to 0.078125
- down_weight: bfloat16 [12800, 5120], P('row'), may hold values from -0.0546875 to 0.0546875
Outputs:
- master_new: float32 [12800, 5120], P('row', ('group', 'col'))
- moment_new: float32 [12800, 5120], P('row', ('group', 'col'))
- second_new: float32 [12800, 5120], P('row', ('group', 'col'))
- prefill: float32 [1024, 5120], P(('group', 'col'), 'row')
The draws below stay inside these ranges and needn't reach their ends.
All inputs are finite; a program needn't handle non-finite values.
Results may differ from the reference program's by a relative error of at most 0.0041.
Values may be sent and summed in bfloat16 or wider, within the bound.
A program may use at most 32 MiB of HBM per device.

```python
import math
import jax
import jax.numpy as jnp

D = 5120
FF = 12800
TOK = 4096
PROMPTS = 1024


def block_scale(stream_key, extent, cuts, least, top_value):
    gain, own = 1.0, jax.random.fold_in(stream_key, 6)
    for position, shards_of in cuts:
        draws = jnp.exp(jax.random.uniform(jax.random.fold_in(own, position), (shards_of,), jnp.float32, least / len(cuts), top_value / len(cuts)))
        gain = gain * jnp.repeat(draws, extent[position] // shards_of).reshape([-1 if axis == position else 1 for axis in range(len(extent))])
    return gain


def gaussian(own_key, shape, deviation, bound, cuts=(), held_as=jnp.bfloat16):
    values = deviation * jax.random.normal(own_key, shape, jnp.float32)
    if cuts:
        values = values * block_scale(own_key, shape, cuts, -0.22, 0.18)
    return jnp.clip(values, -bound, bound).astype(held_as)


def setup_inputs(seed: int = 0) -> dict:
    arg_keys = jax.random.split(jax.random.key(seed), 9)
    return {
        "tokens": gaussian(arg_keys[0], (TOK, D), 1.0, 6.0, ((0, 64), (1, 16))),
        "cotangent": gaussian(arg_keys[1], (TOK, FF), (TOK ** -0.5), 0.09375, ((0, 16), (1, 64))),
        "master": gaussian(arg_keys[2], (FF, D), D ** -0.5, 0.078125, ((0, 64), (1, 16)), jnp.float32),
        "moment": gaussian(arg_keys[3], (FF, D), 1.0, 6.0, ((0, 64), (1, 16)), jnp.float32),
        "second": jnp.clip(jnp.exp(math.log(4.0) - 3.6888794 * jax.random.uniform(arg_keys[4], (FF, D), jnp.float32) ** block_scale(arg_keys[4], (FF, D), ((0, 64), (1, 16)), -0.2, 0.2)), 0.1, 4.0),
        "prompts": gaussian(arg_keys[5], (PROMPTS, D), 1.0, 6.0, ((0, 16),)),
        "up_weight": gaussian(arg_keys[6], (FF, D), D ** -0.5, 0.078125, ((0, 64),)),
        "down_weight": gaussian(arg_keys[7], (FF, D), FF ** -0.5, 0.0546875, ((0, 64),)),
    }


beta_first = 0.9
beta_second = 0.95
learn_rate = 0.002
weight_decay = 0.1
epsilon = 1e-08
first_bias = 1.0 - 0.9 ** 10
second_bias = 1.0 - 0.95 ** 10

def adam_update(gradient, master, moment, second):
    moment_new = beta_first * moment + (1.0 - beta_first) * gradient
    second_new = beta_second * second + (1.0 - beta_second) * gradient * gradient
    direction = moment_new / first_bias / (jnp.sqrt(second_new / second_bias) + epsilon)
    master_new = master - learn_rate * (direction + weight_decay * master)
    return (master_new, moment_new, second_new)

def reference(tokens, cotangent, master, moment, second, prompts, up_weight, down_weight):
    gradient = jnp.dot(cotangent.T, tokens, preferred_element_type=jnp.float32)
    master_new, moment_new, second_new = adam_update(gradient, master, moment, second)
    refreshed = master_new.astype(jnp.bfloat16)
    gate_pre = jnp.dot(prompts, refreshed.T, preferred_element_type=jnp.float32)
    up_pre = jnp.dot(prompts, up_weight.T, preferred_element_type=jnp.float32)
    hidden = (jax.nn.silu(gate_pre) * up_pre).astype(jnp.bfloat16)
    prefill = jnp.dot(hidden, down_weight, preferred_element_type=jnp.float32)
    return (master_new, moment_new, second_new, prefill)
```

```python
import functools

import jax
import jax.numpy as jnp
from jax import lax
from jax.experimental import pallas as pl
from jax.experimental.pallas import tpu as pltpu
from jax.sharding import Mesh
from jax.sharding import PartitionSpec as P

AXES = ("yh", "z", "yl", "x", "core")
ROW = ("z", "yl")
GC = ("yh", "x", "core")
NZ = 32
MESH = pl.DeviceIdType.MESH
f32 = jnp.float32
bf16 = jnp.bfloat16

beta_first = 0.9
beta_second = 0.95
learn_rate = 0.002
weight_decay = 0.1
epsilon = 1e-08
first_bias = 1.0 - 0.9**10
second_bias = 1.0 - 0.95**10


def adam_update(gradient, master, moment, second):
    moment_new = beta_first * moment + (1.0 - beta_first) * gradient
    second_new = beta_second * second + (1.0 - beta_second) * gradient * gradient
    direction = moment_new / first_bias / (jnp.sqrt(second_new / second_bias) + epsilon)
    master_new = master - learn_rate * (direction + weight_decay * master)
    return (master_new, moment_new, second_new)


def wrap(v, n):
    return lax.rem(v + 4 * n, n)


def nt(a, b):
    return lax.dot_general(a, b, (((1,), (1,)), ((), ())), preferred_element_type=f32)


def nn(a, b):
    return jnp.dot(a, b, preferred_element_type=f32)


def kernel(
    tok_ref, cot_ref, master_hbm, moment_hbm, second_hbm, prompts_hbm, up_hbm, down_hbm,
    master_out, moment_out, second_out, prefill_out,
    master_v, moment_v, second_v, prompts_v, up_v, down_v, dperm,
    tsib, csib, tok_all, cs_send, cot_all, p_all,
    gsend, grecv, rsend, rrecv, rcat,
    gp32, gps, gpr, y32, ysend, yrecv, a32, asend, arecv, b32, bsend, brecv,
    loc_sem, d2d_s, d2d_r, js, jr, hs, hr, fs, fr,
    c1s, c1r, c2s, c2r, xs, xr, x2s, x2r, cfs, cfr,
    ps, pr, gs, gr, ys, yr, as_, ar, bs, br,
):
    yh, z, yl, x, c = (lax.axis_index(a) for a in AXES)
    h = yh * 4 + x
    zh, zl = z // 4, lax.rem(z, 4)
    sib = {"core": 1 - c}
    yn = {"yl": 1 - yl}
    sends = []

    def remote(src, dst, ssem, rsem, peer):
        return pltpu.make_async_remote_copy(
            src_ref=src, dst_ref=dst, send_sem=ssem, recv_sem=rsem,
            device_id=peer, device_id_type=MESH,
        )

    loads = []
    for n, (a, b) in enumerate(
        ((prompts_hbm, prompts_v), (master_hbm, master_v), (moment_hbm, moment_v),
         (second_hbm, second_v), (down_hbm, down_v), (up_hbm, up_v))
    ):
        cp = pltpu.make_async_copy(a, b, loc_sem.at[n])
        cp.start()
        loads.append(cp)

    def chip_peer(k):
        o = lax.rem(h + k, 8)
        return o, {"yh": o // 4, "x": lax.rem(o, 4)}

    def near_peer(k):
        o = lax.rem(zl + k, 4)
        return o, {"z": zh * 4 + o}

    barrier = pltpu.get_barrier_semaphore()
    peers = [sib, yn]
    peers += [{"z": wrap(z + d, NZ)} for d in (1, -1, 2, -2)]
    peers += [near_peer(k)[1] for k in range(1, 4)]
    peers += [chip_peer(k)[1] for k in range(1, 8)]
    for peer in peers:
        pl.semaphore_signal(barrier, inc=1, device_id=peer, device_id_type=MESH)
    pl.semaphore_wait(barrier, len(peers))

    tok_d2d = remote(tok_ref, tsib, d2d_s.at[0], d2d_r.at[0], sib)
    cot_d2d = remote(cot_ref, csib, d2d_s.at[0], d2d_r.at[0], sib)

    def block(d):
        return wrap(z - d, NZ)

    order = {0: 0}
    for d in range(1, 16):
        order[d] = len(order)
        order[-d] = len(order)
    order[16] = len(order)

    def fwd(d):
        b = tok_all.at[block(d)]
        return remote(b, b, fs.at[order[d]], fr.at[order[d]], sib)

    def jump(dr, k):
        b = tok_all.at[block(dr * 2 * k)]
        i = 0 if dr > 0 else 1
        return remote(b, b, js.at[i, k], jr.at[i, k], {"z": wrap(z + 2 * dr, NZ)})

    def jump_in(dr, k):
        b = tok_all.at[block(dr * 2 * (k + 1))]
        i = 0 if dr > 0 else 1
        return remote(b, b, js.at[i, k], jr.at[i, k], {"z": wrap(z + 2 * dr, NZ)})

    def hop(dr, k):
        b = tok_all.at[block(dr * 2 * k)]
        i = 0 if dr > 0 else 1
        return remote(b, b, hs.at[i, k], hr.at[i, k], {"z": wrap(z + dr, NZ)})

    def hop_in(dr, k):
        b = tok_all.at[block(dr * (2 * k + 1))]
        i = 0 if dr > 0 else 1
        return remote(b, b, hs.at[i, k], hr.at[i, k], {"z": wrap(z + dr, NZ)})

    def njump(dr):
        return 8 if dr > 0 else 7

    def prompt_send(k):
        o, peer = chip_peer(k)
        return remote(
            prompts_v.at[:, pl.ds(pl.multiple_of(o * 640, 128), 640)],
            p_all.at[h], ps.at[k], pr.at[k], peer,
        )

    def send_prompts():
        loads[0].wait()
        for k in range(1, 8):
            prompt_send(k).start()
        p_all[h] = prompts_v[:, pl.ds(pl.multiple_of(h * 640, 128), 640)]

    hy = (1 - yh) * 4 + x

    def hx(sel, d):
        return (yh if sel == 0 else 1 - yh) * 4 + wrap(x + d, 4)

    cot1 = remote(cs_send, cot_all.at[h, yl], c1s, c1r, yn)
    cot1_in = remote(cs_send, cot_all.at[h, 1 - yl], c1s, c1r, yn)
    cot2 = remote(cot_all.at[h], cot_all.at[h], c2s, c2r, {"yh": 1 - yh})
    cot2_in = remote(cot_all.at[hy], cot_all.at[hy], c2s, c2r, {"yh": 1 - yh})

    def xsend(sel, dr):
        b = cot_all.at[hx(sel, 0)]
        i = 0 if dr > 0 else 1
        return remote(b, b, xs.at[i, sel], xr.at[i, sel], {"x": wrap(x + dr, 4)})

    def xin(sel, dr):
        b = cot_all.at[hx(sel, -dr)]
        i = 0 if dr > 0 else 1
        return remote(b, b, xs.at[i, sel], xr.at[i, sel], {"x": wrap(x + dr, 4)})

    def x2send(sel, dr):
        i = 0 if dr > 0 else 1
        b = cot_all.at[hx(sel, -dr), i]
        return remote(b, b, x2s.at[i, sel], x2r.at[i, sel], {"x": wrap(x + dr, 4)})

    def x2in(sel, dr):
        i = 0 if dr > 0 else 1
        b = cot_all.at[hx(sel, -2 * dr), i]
        return remote(b, b, x2s.at[i, sel], x2r.at[i, sel], {"x": wrap(x + dr, 4)})

    def cfwd(n):
        if n == 0:
            b = cot_all.at[h]
        elif n == 1:
            b = cot_all.at[hy]
        elif n < 6:
            sel, i = (n - 2) // 2, (n - 2) % 2
            b = cot_all.at[hx(sel, -1 if i == 0 else 1)]
        else:
            sel, i = (n - 6) // 2, (n - 6) % 2
            b = cot_all.at[hx(sel, 2), i]
        return remote(b, b, cfs.at[n], cfr.at[n], sib)

    @pl.when(c == 1)
    def _():
        cot_d2d.start()
        tok_d2d.wait_recv()
        mine, other = tok_ref[...], tsib[...]
        tok_all[z] = jnp.concatenate(
            [other[:, :256], mine[:, :256], other[:, 256:], mine[:, 256:]], axis=1
        )
        for dr in (1, -1):
            jump(dr, 0).start()
            hop(dr, 0).start()
        fwd(0).start()
        for k in range(1, 9):
            for dr in (1, -1):
                if k <= njump(dr):
                    jump_in(dr, k - 1).wait_recv()
                    if k < njump(dr):
                        jump(dr, k).start()
                    if k < 8:
                        hop(dr, k).start()
                    fwd(dr * 2 * k).start()
            for dr in (1, -1):
                hop_in(dr, k - 1).wait_recv()
                fwd(dr * (2 * k - 1)).start()
            if k == 2:
                send_prompts()
        for n in range(10):
            cfwd(n).wait_recv()

    @pl.when(c == 0)
    def _():
        tok_d2d.start()
        cot_d2d.wait_recv()
        for core, src in ((0, cot_ref), (1, csib)):
            v = src[...]
            even = jnp.concatenate([v[:, :64], v[:, 128:192]], axis=1)
            odd = jnp.concatenate([v[:, 64:128], v[:, 192:]], axis=1)
            first = yl == 0
            cot_all[h, yl, core] = jnp.where(first, even, odd)
            cs_send[core] = jnp.where(first, odd, even)
        cot1.start()
        cot1_in.wait_recv()
        cot2.start()
        for dr in (1, -1):
            xsend(0, dr).start()
        cfwd(0).start()
        cot2_in.wait_recv()
        for dr in (1, -1):
            xsend(1, dr).start()
        cfwd(1).start()
        for sel in range(2):
            for i, dr in enumerate((1, -1)):
                xin(sel, dr).wait_recv()
                x2send(sel, dr).start()
                cfwd(2 + 2 * sel + i).start()
        send_prompts()
        for sel in range(2):
            for i, dr in enumerate((1, -1)):
                x2in(sel, dr).wait_recv()
                cfwd(6 + 2 * sel + i).start()
        for d in order:
            fwd(d).wait_recv()

    first_core = c == 0

    def gradient(part):
        wide = jnp.zeros((200, 256), f32)
        rest = jnp.zeros((200, 128), f32)
        for o in range(8):
            lhs = jnp.concatenate([cot_all[o, part, 0], cot_all[o, part, 1]], axis=1)
            t = tok_all[4 * o : 4 * o + 4, :, pl.ds(pl.multiple_of(c * 256, 256), 256)]
            wide += nn(lhs, t.reshape(256, 256))
            rest += nn(lhs, tok_all[4 * o : 4 * o + 4, :, 512:640].reshape(256, 128))
        return wide, jnp.where(first_core, rest[:, :64], rest[:, 64:])

    wide, rest = gradient(1 - yl)
    gsend[:, :256] = wide.astype(bf16)
    gsend[:, 256:] = rest.astype(bf16)
    gcp = remote(gsend, grecv, d2d_s.at[1], d2d_r.at[1], yn)
    gcp.start()
    wide, rest = gradient(yl)
    for n in (1, 2, 3, 4):
        loads[n].wait()
    for r in range(64):
        zz, l = r // 2, r % 2
        at = ((l * 4 + zz % 4) * 8 + zz // 4) * 80
        dperm[:, at : at + 80] = down_v[:, 80 * r : 80 * r + 80]
    gcp.wait_recv()
    for part, lanes in ((wide, slice(0, 256)), (rest, slice(256, 320))):
        total = part + grecv[:, lanes].astype(f32)
        new = adam_update(total, master_v[:, lanes], moment_v[:, lanes], second_v[:, lanes])
        master_out[:, lanes] = new[0]
        moment_out[:, lanes] = new[1]
        second_out[:, lanes] = new[2]
        rsend[:, lanes] = new[0].astype(bf16)
    rcp = remote(rsend, rrecv, d2d_s.at[2], d2d_r.at[2], sib)
    rcp.start()
    for k in range(1, 8):
        prompt_send(k).wait_recv()
    rcp.wait_recv()
    mine, other = rsend[...], rrecv[...]
    rcat[:, :320] = jnp.where(first_core, mine, other)
    rcat[:, 320:] = jnp.where(first_core, other, mine)

    for o in range(8):
        v = nt(p_all[o], rcat[...])
        gp32[o] = v
        gps[o] = v.astype(bf16)

    def gate_send(k):
        o, peer = chip_peer(k)
        return remote(gps.at[o], gpr.at[h], gs.at[k], gr.at[k], peer)

    for k in (4, 2, 6, 1, 3, 5, 7):
        gate_send(k).start()
    loads[5].wait()
    up_pre = nt(prompts_v[...], up_v[...])
    gate = gp32[h]
    for k in range(1, 8):
        gate_send(k).wait_recv()
        gate += gpr[wrap(h - k, 8)].astype(f32)
    hidden = (gate / (1.0 + jnp.exp(-gate)) * up_pre).astype(bf16)

    def half(l):
        return dperm[:, pl.ds(pl.multiple_of(l * 2560, 128), 2560)]

    ysend[...] = nn(hidden, half(1 - yl)).astype(bf16)
    ycp = remote(ysend, yrecv, ys, yr, yn)
    ycp.start()
    y32[...] = nn(hidden, half(yl))
    ycp.wait_recv()
    for o in range(4):
        v = y32[:, 640 * o : 640 * o + 640] + yrecv[:, 640 * o : 640 * o + 640].astype(f32)
        a32[o] = v
        asend[o] = v.astype(bf16)

    def near_send(k):
        o, peer = near_peer(k)
        return remote(asend.at[o], arecv.at[zl], as_.at[k], ar.at[k], peer)

    for k in range(1, 4):
        near_send(k).start()
    total = a32[zl]
    for k in range(1, 4):
        near_send(k).wait_recv()
        total += arecv[wrap(zl - k, 4)].astype(f32)
    for o in range(8):
        v = total[:, 80 * o : 80 * o + 80]
        b32[o] = v
        bsend[o] = v.astype(bf16)

    def far_send(k):
        o = lax.rem(zh + k, 8)
        return remote(bsend.at[o], brecv.at[zh], bs.at[k], br.at[k], {"z": o * 4 + zl})

    for k in (4, 3, 5, 2, 6, 1, 7):
        far_send(k).start()
    total = b32[zh]
    for k in (1, 7, 2, 6, 3, 5, 4):
        far_send(k).wait_recv()
        total += brecv[wrap(zh - k, 8)].astype(f32)
    prefill_out[...] = total

    @pl.when(c == 1)
    def _():
        cot_d2d.wait_send()
        for dr in (1, -1):
            for k in range(8):
                if k < njump(dr):
                    jump(dr, k).wait_send()
                hop(dr, k).wait_send()
        for d in order:
            fwd(d).wait_send()

    @pl.when(c == 0)
    def _():
        tok_d2d.wait_send()
        cot1.wait_send()
        cot2.wait_send()
        for sel in range(2):
            for dr in (1, -1):
                xsend(sel, dr).wait_send()
                x2send(sel, dr).wait_send()
        for n in range(10):
            cfwd(n).wait_send()

    for cp in (gcp, rcp, ycp):
        cp.wait_send()
    for k in range(1, 8):
        prompt_send(k).wait_send()
        gate_send(k).wait_send()
        far_send(k).wait_send()
    for k in range(1, 4):
        near_send(k).wait_send()


def shards(tokens, cotangent, master, moment, second, prompts, up_weight, down_weight):
    V, D = pltpu.VMEM, pltpu.SemaphoreType.DMA
    vmem = pl.BlockSpec(memory_space=pltpu.VMEM)
    hbm = pl.BlockSpec(memory_space=pl.ANY)
    out = jax.ShapeDtypeStruct
    return pl.pallas_call(
        kernel,
        out_shape=(
            out((200, 320), f32), out((200, 320), f32), out((200, 320), f32), out((64, 80), f32),
        ),
        in_specs=[vmem] * 2 + [hbm] * 6,
        out_specs=[vmem] * 4,
        scratch_shapes=[
            V((200, 320), f32), V((200, 320), f32), V((200, 320), f32),
            V((64, 5120), bf16), V((200, 5120), bf16), V((200, 5120), bf16), V((200, 5120), bf16),
            V((64, 320), bf16), V((200, 256), bf16), V((32, 64, 640), bf16),
            V((2, 200, 128), bf16), V((8, 2, 2, 200, 128), bf16), V((8, 64, 640), bf16),
            V((200, 320), bf16), V((200, 320), bf16), V((200, 320), bf16), V((200, 320), bf16),
            V((200, 640), bf16),
            V((8, 64, 200), f32), V((8, 64, 200), bf16), V((8, 64, 200), bf16),
            V((64, 2560), f32), V((64, 2560), bf16), V((64, 2560), bf16),
            V((4, 64, 640), f32), V((4, 64, 640), bf16), V((4, 64, 640), bf16),
            V((8, 64, 80), f32), V((8, 64, 80), bf16), V((8, 64, 80), bf16),
            D((6,)), D((3,)), D((3,)), D((2, 8)), D((2, 8)), D((2, 8)), D((2, 8)),
            D((32,)), D((32,)),
            D(()), D(()), D(()), D(()), D((2, 2)), D((2, 2)), D((2, 2)), D((2, 2)),
            D((10,)), D((10,)),
            D((8,)), D((8,)), D((8,)), D((8,)), D(()), D(()), D((4,)), D((4,)), D((8,)), D((8,)),
        ],
        compiler_params=pltpu.CompilerParams(
            collective_id=0, has_side_effects=True, vmem_limit_bytes=56 * 1024 * 1024
        ),
    )(tokens, cotangent.T, master, moment, second, prompts, up_weight, down_weight)


def solution(mesh):
    split = Mesh(mesh.devices.reshape(2, NZ, 2, 4, 2), AXES)
    tile, rows = P(ROW, GC), P(GC, ROW)
    return jax.shard_map(
        shards,
        mesh=split,
        in_specs=(tile, rows, tile, tile, tile, P(GC, None), P(ROW, None), P(ROW, None)),
        out_specs=(tile, tile, tile, rows),
        check_vma=False,
    )
```

```python
import functools

import jax
import jax.numpy as jnp
from jax import lax
from jax.experimental import pallas as pl
from jax.experimental.pallas import tpu as pltpu
from jax.sharding import Mesh
from jax.sharding import PartitionSpec as P

AXES = ("yh", "z", "yl", "x", "core")
ROW = ("z", "yl")
GC = ("yh", "x", "core")
NZ = 32
JUMP = 2
CH = 4
MESH = pl.DeviceIdType.MESH
f32 = jnp.float32
bf16 = jnp.bfloat16

beta_first = 0.9
beta_second = 0.95
learn_rate = 0.002
weight_decay = 0.1
epsilon = 1e-08
first_bias = 1.0 - 0.9**10
second_bias = 1.0 - 0.95**10


def adam_update(gradient, master, moment, second):
    moment_new = beta_first * moment + (1.0 - beta_first) * gradient
    second_new = beta_second * second + (1.0 - beta_second) * gradient * gradient
    direction = moment_new / first_bias / (jnp.sqrt(second_new / second_bias) + epsilon)
    master_new = master - learn_rate * (direction + weight_decay * master)
    return (master_new, moment_new, second_new)


def wrap(v, n):
    return lax.rem(v + 4 * n, n)


def nt(a, b):
    return lax.dot_general(a, b, (((1,), (1,)), ((), ())), preferred_element_type=f32)


def nn(a, b):
    return jnp.dot(a, b, preferred_element_type=f32)


def kernel(
    tok_hbm, cot_hbm, master_hbm, moment_hbm, second_hbm, prompts_hbm, up_hbm, down_hbm,
    master_hout, moment_hout, second_hout, prefill_out,
    master_out, moment_out, second_out,
    tok_ref, cot_ref, master_v, moment_v, second_v, prompts_v, up_v, down_v, dperm, dother,
    tsib, csib, tok_all, cs_send, cot_all, p_all,
    gsend, grecv, rsend, rrecv, rcat,
    gp32, gps, gpr, hid, hrecv, a32, asend, arecv, b32, bsend, brecv,
    loc_sem, st_sem, d2d_s, d2d_r, js, jr, hs, hr, fs, fr,
    c1s, c1r, c2s, c2r, xs, xr, x2s, x2r, cfs, cfr,
    ps, pr, gs, gr, ds_, dr_, as_, ar, bs, br,
):
    yh, z, yl, x, c = (lax.axis_index(a) for a in AXES)
    h = yh * 4 + x
    zh, zl = z // 4, lax.rem(z, 4)
    sib = {"core": 1 - c}
    yn = {"yl": 1 - yl}
    sends = []

    def remote(src, dst, ssem, rsem, peer):
        return pltpu.make_async_remote_copy(
            src_ref=src, dst_ref=dst, send_sem=ssem, recv_sem=rsem,
            device_id=peer, device_id_type=MESH,
        )

    loads = []
    for n, (a, b) in enumerate(
        ((prompts_hbm, prompts_v), (master_hbm, master_v), (moment_hbm, moment_v),
         (second_hbm, second_v), (down_hbm, down_v), (up_hbm, up_v),
         (tok_hbm, tok_ref), (cot_hbm, cot_ref))
    ):
        cp = pltpu.make_async_copy(a, b, loc_sem.at[n])
        loads.append(cp)
    for n in (6, 7, 0, 4, 1, 2, 3, 5):
        loads[n].start()

    def chip_peer(k):
        o = lax.rem(h + k, 8)
        return o, {"yh": o // 4, "x": lax.rem(o, 4)}

    def prompt_peer(k):
        o = lax.rem(h + k, 8)
        return o, {"yh": o // 4, "x": lax.rem(o, 4), "yl": lax.rem(yl + yh + o // 4, 2)}

    def near_peer(s, k):
        u = wrap(z + 2 * s, NZ)
        to = wrap(u // 4 * 4 + lax.rem(u + k, 4) - 2 * s, NZ)
        return lax.rem(to, 4), {"z": to}

    barrier = pltpu.get_barrier_semaphore()
    peers = [sib, yn]
    peers += [{"z": wrap(z + d, NZ)} for d in (1, -1, 2, -2)]
    peers += [near_peer(s, k)[1] for s in range(2) for k in range(1, 4)]
    peers += [chip_peer(k)[1] for k in range(1, 8)]
    peers += [prompt_peer(k)[1] for k in range(1, 8)]
    for peer in peers:
        pl.semaphore_signal(barrier, inc=1, device_id=peer, device_id_type=MESH)
    pl.semaphore_wait(barrier, len(peers))
    loads[6].wait()
    loads[7].wait()

    tok_d2d = remote(tok_ref, tsib, d2d_s.at[0], d2d_r.at[0], sib)
    cot_d2d = remote(cot_ref, csib, d2d_s.at[0], d2d_r.at[0], sib)

    def block(d):
        return wrap(z - d, NZ)

    order = {0: 0}
    for d in range(1, 16):
        order[d] = len(order)
        order[-d] = len(order)
    order[16] = len(order)

    def fwd(d):
        b = tok_all.at[block(d)]
        return remote(b, b, fs.at[order[d]], fr.at[order[d]], sib)

    rows = 64 // CH
    steps = 16 // JUMP

    def side(dr):
        return 0 if dr > 0 else 1

    def piece(d, ch):
        return tok_all.at[block(d), pl.ds(rows * ch, rows)]

    def jump(dr, k, ch):
        b, i = piece(dr * JUMP * k, ch), side(dr)
        return remote(b, b, js.at[i, k], jr.at[i, k, ch], {"z": wrap(z + JUMP * dr, NZ)})

    def jump_in(dr, k, ch):
        b, i = piece(dr * JUMP * (k + 1), ch), side(dr)
        return remote(b, b, js.at[i, k], jr.at[i, k, ch], {"z": wrap(z + JUMP * dr, NZ)})

    def jump_out(dr, k):
        b, i = tok_all.at[block(dr * JUMP * k)], side(dr)
        return remote(b, b, js.at[i, k], jr.at[i, k, 0], {"z": wrap(z + JUMP * dr, NZ)})

    def hop(dr, k, ch):
        b, i = piece(dr * 2 * k, ch), side(dr)
        return remote(b, b, hs.at[i, k], hr.at[i, k], {"z": wrap(z + dr, NZ)})

    def hop_out(dr, k):
        b, i = tok_all.at[block(dr * 2 * k)], side(dr)
        return remote(b, b, hs.at[i, k], hr.at[i, k], {"z": wrap(z + dr, NZ)})

    def hop_in(dr, k):
        b, i = tok_all.at[block(dr * (2 * k + 1))], side(dr)
        return remote(b, b, hs.at[i, k], hr.at[i, k], {"z": wrap(z + dr, NZ)})

    def njump(dr):
        return steps if dr > 0 else steps - 1

    def prompt_send(k):
        o, peer = prompt_peer(k)
        return remote(
            prompts_v.at[:, pl.ds(pl.multiple_of(o * 640, 128), 640)],
            p_all.at[h], ps.at[k], pr.at[k], peer,
        )

    def send_prompts():
        loads[0].wait()
        for k in range(1, 8):
            prompt_send(k).start()
        p_all[h] = prompts_v[:, pl.ds(pl.multiple_of(h * 640, 128), 640)]

    hy = (1 - yh) * 4 + x

    def hx(sel, d):
        return (yh if sel == 0 else 1 - yh) * 4 + wrap(x + d, 4)

    cot1 = remote(cs_send, cot_all.at[h, yl], c1s, c1r, yn)
    cot1_in = remote(cs_send, cot_all.at[h, 1 - yl], c1s, c1r, yn)
    cot2 = remote(cot_all.at[h], cot_all.at[h], c2s, c2r, {"yh": 1 - yh})
    cot2_in = remote(cot_all.at[hy], cot_all.at[hy], c2s, c2r, {"yh": 1 - yh})

    def xsend(sel, dr):
        b = cot_all.at[hx(sel, 0)]
        i = 0 if dr > 0 else 1
        return remote(b, b, xs.at[i, sel], xr.at[i, sel], {"x": wrap(x + dr, 4)})

    def xin(sel, dr):
        b = cot_all.at[hx(sel, -dr)]
        i = 0 if dr > 0 else 1
        return remote(b, b, xs.at[i, sel], xr.at[i, sel], {"x": wrap(x + dr, 4)})

    def x2send(sel, dr):
        i = 0 if dr > 0 else 1
        b = cot_all.at[hx(sel, -dr), i]
        return remote(b, b, x2s.at[i, sel], x2r.at[i, sel], {"x": wrap(x + dr, 4)})

    def x2in(sel, dr):
        i = 0 if dr > 0 else 1
        b = cot_all.at[hx(sel, -2 * dr), i]
        return remote(b, b, x2s.at[i, sel], x2r.at[i, sel], {"x": wrap(x + dr, 4)})

    def cfwd(n):
        if n == 0:
            b = cot_all.at[h]
        elif n == 1:
            b = cot_all.at[hy]
        elif n < 6:
            sel, i = (n - 2) // 2, (n - 2) % 2
            b = cot_all.at[hx(sel, -1 if i == 0 else 1)]
        else:
            sel, i = (n - 6) // 2, (n - 6) % 2
            b = cot_all.at[hx(sel, 2), i]
        return remote(b, b, cfs.at[n], cfr.at[n], sib)

    down_y = remote(dperm.at[1 - yl], dother, ds_.at[0], dr_.at[0], yn)
    down_own = remote(dperm.at[yl], dperm.at[yl], ds_.at[1], dr_.at[1], sib)
    down_sib = remote(dother, dother, ds_.at[2], dr_.at[2], sib)

    @pl.when(c == 1)
    def _():
        cot_d2d.start()
        tok_d2d.wait_recv()
        mine, other = tok_ref[...], tsib[...]
        tok_all[z] = jnp.concatenate(
            [other[:, :256], mine[:, :256], other[:, 256:], mine[:, 256:]], axis=1
        )
        for ch in range(CH):
            for dr in (1, -1):
                jump(dr, 0, ch).start()
                if JUMP == 2:
                    hop(dr, 0, ch).start()
        fwd(0).start()
        for k in range(1, steps + 1):
            for ch in range(CH):
                for dr in (1, -1):
                    if k > njump(dr):
                        continue
                    jump_in(dr, k - 1, ch).wait_recv()
                    if k < njump(dr):
                        jump(dr, k, ch).start()
                    if JUMP == 2 and k < steps:
                        hop(dr, k, ch).start()
                    if ch == CH - 1:
                        fwd(dr * JUMP * k).start()
            if JUMP == 2:
                for dr in (1, -1):
                    hop_in(dr, k - 1).wait_recv()
                    fwd(dr * (2 * k - 1)).start()
            if k == steps // 4:
                send_prompts()
        for n in range(10):
            cfwd(n).wait_recv()

    @pl.when(c == 0)
    def _():
        tok_d2d.start()
        cot_d2d.wait_recv()
        for core, src in ((0, cot_ref), (1, csib)):
            v = src[...]
            even = jnp.concatenate([v[:, :64], v[:, 128:192]], axis=1)
            odd = jnp.concatenate([v[:, 64:128], v[:, 192:]], axis=1)
            first = yl == 0
            cot_all[h, yl, core] = jnp.where(first, even, odd)
            cs_send[core] = jnp.where(first, odd, even)
        cot1.start()
        cot1_in.wait_recv()
        cot2.start()
        for dr in (1, -1):
            xsend(0, dr).start()
        cfwd(0).start()
        cot2_in.wait_recv()
        for dr in (1, -1):
            xsend(1, dr).start()
        cfwd(1).start()
        for sel in range(2):
            for i, dr in enumerate((1, -1)):
                xin(sel, dr).wait_recv()
                x2send(sel, dr).start()
                cfwd(2 + 2 * sel + i).start()
        send_prompts()
        for sel in range(2):
            for i, dr in enumerate((1, -1)):
                x2in(sel, dr).wait_recv()
                cfwd(6 + 2 * sel + i).start()
        loads[4].wait()
        for r in range(64):
            zz, l = r // 2, r % 2
            at, part = zz % 4 * 640, zz // 4
            dperm[l, :, at + 64 * part : at + 64 * part + 64] = down_v[:, 80 * r : 80 * r + 64]
            at += 512 + 16 * part
            dperm[l, :, at : at + 16] = down_v[:, 80 * r + 64 : 80 * r + 80]
        down_y.start()
        down_own.start()
        for d in order:
            fwd(d).wait_recv()

    first_core = c == 0

    def gradient(part):
        wide = jnp.zeros((200, 256), f32)
        rest = jnp.zeros((200, 128), f32)
        for o in range(8):
            lhs = jnp.concatenate([cot_all[o, part, 0], cot_all[o, part, 1]], axis=1)
            t = tok_all[4 * o : 4 * o + 4, :, pl.ds(pl.multiple_of(c * 256, 256), 256)]
            wide += nn(lhs, t.reshape(256, 256))
            rest += nn(lhs, tok_all[4 * o : 4 * o + 4, :, 512:640].reshape(256, 128))
        return wide, jnp.where(first_core, rest[:, :64], rest[:, 64:])

    wide, rest = gradient(1 - yl)
    gsend[:, :256] = wide.astype(bf16)
    gsend[:, 256:] = rest.astype(bf16)
    gcp = remote(gsend, grecv, d2d_s.at[1], d2d_r.at[1], yn)
    gcp.start()
    wide, rest = gradient(yl)
    for n in (1, 2, 3):
        loads[n].wait()
    gcp.wait_recv()
    for part, lanes in ((wide, slice(0, 256)), (rest, slice(256, 320))):
        total = part + grecv[:, lanes].astype(f32)
        new = adam_update(total, master_v[:, lanes], moment_v[:, lanes], second_v[:, lanes])
        master_out[:, lanes] = new[0]
        moment_out[:, lanes] = new[1]
        second_out[:, lanes] = new[2]
        rsend[:, lanes] = new[0].astype(bf16)
    stores = []
    for n, (a, b) in enumerate(
        ((master_out, master_hout), (moment_out, moment_hout), (second_out, second_hout))
    ):
        stores.append(pltpu.make_async_copy(a, b, st_sem.at[n]))
    rcp = remote(rsend, rrecv, d2d_s.at[2], d2d_r.at[2], sib)
    rcp.start()
    for cp in stores:
        cp.start()

    @pl.when(c == 0)
    def _():
        down_y.wait_recv()
        down_sib.start()

    for k in range(1, 8):
        prompt_send(k).wait_recv()
    rcp.wait_recv()
    mine, other = rsend[...], rrecv[...]
    rcat[:, :320] = jnp.where(first_core, mine, other)
    rcat[:, 320:] = jnp.where(first_core, other, mine)

    for o in range(8):
        v = nt(p_all[o], rcat[...])
        gp32[o] = v
        gps[o] = v.astype(bf16)

    def gate_send(k):
        o, peer = chip_peer(k)
        return remote(gps.at[o], gpr.at[h], gs.at[k], gr.at[k], peer)

    for k in (4, 2, 6, 1, 3, 5, 7):
        gate_send(k).start()
    loads[5].wait()
    up_pre = nt(prompts_v[...], up_v[...])
    gate = gp32[h]
    for k in range(1, 8):
        gate_send(k).wait_recv()
        gate += gpr[wrap(h - k, 8)].astype(f32)
    hidden = (gate / (1.0 + jnp.exp(-gate)) * up_pre).astype(bf16)
    hid[...] = hidden
    hcp = remote(hid, hrecv, d2d_s.at[3], d2d_r.at[3], yn)
    hcp.start()

    @pl.when(c == 1)
    def _():
        down_own.wait_recv()
        down_sib.wait_recv()

    for o in range(4):
        a32[o] = nn(hidden, dperm[yl, :, 640 * o : 640 * o + 640])
    hcp.wait_recv()
    hidden = hrecv[...]

    def near_send(s, k):
        o, peer = near_peer(s, k)
        part = pl.ds(32 * s, 32)
        return remote(asend.at[o, part], arecv.at[k - 1, part], as_.at[s, k], ar.at[s, k], peer)

    for o in range(4):
        v = a32[o] + nn(hidden, dother[:, 640 * o : 640 * o + 640])
        a32[o] = v
        asend[o] = v.astype(bf16)
    for s in range(2):
        for k in (2, 1, 3):
            near_send(s, k).start()

    def far_send(k):
        o = lax.rem(zh + k, 8)
        return remote(bsend.at[o], brecv.at[k - 1], bs.at[k], br.at[k], {"z": o * 4 + zl})

    for s in range(2):
        part = slice(32 * s, 32 * s + 32)
        total = a32[zl, part]
        for k in range(1, 4):
            near_send(s, k).wait_recv()
            total += arecv[k - 1, part].astype(f32)
        a32[zl, part] = total
    lane = lax.broadcasted_iota(jnp.int32, (32, 128), 1)
    for o in range(4):
        top = a32[zl, :32, 128 * o : 128 * o + 128]
        low = a32[zl, 32:, 128 * o : 128 * o + 128]
        even = jnp.where(lane < 64, top, pltpu.roll(low, 64, 1))
        odd = jnp.where(lane < 64, pltpu.roll(top, 64, 1), low)
        b32[2 * o, :32], b32[2 * o + 1, :32] = even, odd
        bsend[2 * o, :32], bsend[2 * o + 1, :32] = even.astype(bf16), odd.astype(bf16)
    last = a32[zl, :, 512:640]
    rolled = [last] + [pltpu.roll(last, 16 * n, 1) for n in range(1, 8)]
    sixteen = lax.broadcasted_iota(jnp.int32, (8, 128), 1) // 16
    for o in range(8):
        v = rolled[-o % 8][:8]
        for q in range(1, 8):
            v = jnp.where(sixteen == q, rolled[(q - o) % 8][8 * q : 8 * q + 8], v)
        b32[o, 32:] = v
        bsend[o, 32:] = v.astype(bf16)
    for k in (4, 3, 5, 2, 6, 1, 7):
        far_send(k).start()
    total = b32[zh]
    for k in (1, 7, 2, 6, 3, 5, 4):
        far_send(k).wait_recv()
        total += brecv[k - 1].astype(f32)
    prefill_out[:32, :64] = total[:32, :64]
    prefill_out[32:, :64] = total[:32, 64:]
    for q in range(8):
        prefill_out[8 * q : 8 * q + 8, 64:] = total[32:, 16 * q : 16 * q + 16]

    @pl.when(c == 1)
    def _():
        cot_d2d.wait_send()
        for dr in (1, -1):
            for k in range(steps):
                if k < njump(dr):
                    jump_out(dr, k).wait_send()
                if JUMP == 2:
                    hop_out(dr, k).wait_send()
        for d in order:
            fwd(d).wait_send()

    @pl.when(c == 0)
    def _():
        tok_d2d.wait_send()
        down_y.wait_send()
        down_own.wait_send()
        down_sib.wait_send()
        cot1.wait_send()
        cot2.wait_send()
        for sel in range(2):
            for dr in (1, -1):
                xsend(sel, dr).wait_send()
                x2send(sel, dr).wait_send()
        for n in range(10):
            cfwd(n).wait_send()

    @pl.when(c == 1)
    def _():
        loads[4].wait()

    for cp in stores:
        cp.wait()
    for cp in (gcp, rcp, hcp):
        cp.wait_send()
    for k in range(1, 8):
        prompt_send(k).wait_send()
        gate_send(k).wait_send()
        far_send(k).wait_send()
    for s in range(2):
        for k in range(1, 4):
            near_send(s, k).wait_send()


def deliver(*refs):
    ins, outs, held, (in_sem, out_sem) = refs[:4], refs[4:8], refs[8:12], refs[12:]
    reads = [pltpu.make_async_copy(ins[n], held[n], in_sem.at[n]) for n in range(4)]
    writes = [pltpu.make_async_copy(held[n], outs[n], out_sem.at[n]) for n in range(4)]
    for cp in reads:
        cp.start()
    for n in range(4):
        reads[n].wait()
        writes[n].start()
    for cp in writes:
        cp.wait()


def shards(tokens, cotangent, master, moment, second, prompts, up_weight, down_weight):
    V, D = pltpu.VMEM, pltpu.SemaphoreType.DMA
    vmem = pl.BlockSpec(memory_space=pltpu.VMEM)
    hbm = pl.BlockSpec(memory_space=pltpu.HBM)
    out = jax.ShapeDtypeStruct
    results = pl.pallas_call(
        kernel,
        out_shape=(
            out((200, 320), f32), out((200, 320), f32), out((200, 320), f32), out((64, 80), f32),
        ),
        in_specs=[hbm] * 8,
        out_specs=[hbm] * 3 + [vmem],
        scratch_shapes=[
            V((200, 320), f32), V((200, 320), f32), V((200, 320), f32),
            V((64, 320), bf16), V((200, 256), bf16),
            V((200, 320), f32), V((200, 320), f32), V((200, 320), f32),
            V((64, 5120), bf16), V((200, 5120), bf16), V((200, 5120), bf16),
            V((2, 200, 2560), bf16), V((200, 2560), bf16),
            V((64, 320), bf16), V((200, 256), bf16), V((32, 64, 640), bf16),
            V((2, 200, 128), bf16), V((8, 2, 2, 200, 128), bf16), V((8, 64, 640), bf16),
            V((200, 320), bf16), V((200, 320), bf16), V((200, 320), bf16), V((200, 320), bf16),
            V((200, 640), bf16),
            V((8, 64, 200), f32), V((8, 64, 200), bf16), V((8, 64, 200), bf16),
            V((64, 200), bf16), V((64, 200), bf16),
            V((4, 64, 640), f32), V((4, 64, 640), bf16), V((3, 64, 640), bf16),
            V((8, 40, 128), f32), V((8, 40, 128), bf16), V((7, 40, 128), bf16),
            D((8,)), D((3,)), D((4,)), D((4,)), D((2, 16)), D((2, 16, CH)), D((2, 8)), D((2, 8)),
            D((32,)), D((32,)),
            D(()), D(()), D(()), D(()), D((2, 2)), D((2, 2)), D((2, 2)), D((2, 2)),
            D((10,)), D((10,)),
            D((8,)), D((8,)), D((8,)), D((8,)), D((3,)), D((3,)),
            D((2, 4)), D((2, 4)), D((8,)), D((8,)),
        ],
        compiler_params=pltpu.CompilerParams(
            collective_id=0, has_side_effects=True, vmem_limit_bytes=65_900_000
        ),
    )(tokens, cotangent.T, master, moment, second, prompts, up_weight, down_weight)
    return pl.pallas_call(
        deliver,
        out_shape=tuple(out(r.shape, f32) for r in results),
        in_specs=[hbm] * 4,
        out_specs=[hbm] * 4,
        scratch_shapes=[V(r.shape, f32) for r in results] + [D((4,)), D((4,))],
        compiler_params=pltpu.CompilerParams(vmem_limit_bytes=65_900_000),
    )(*results)


def solution(mesh):
    split = Mesh(mesh.devices.reshape(2, NZ, 2, 4, 2), AXES)
    tile, rows = P(ROW, GC), P(GC, ROW)
    return jax.shard_map(
        shards,
        mesh=split,
        in_specs=(tile, rows, tile, tile, tile, P(GC, None), P(ROW, None), P(ROW, None)),
        out_specs=(tile, tile, tile, rows),
        check_vma=False,
    )
```

```python
import functools

import jax
import jax.numpy as jnp
from jax import lax
from jax.experimental import pallas as pl
from jax.experimental.pallas import tpu as pltpu
from jax.sharding import Mesh
from jax.sharding import PartitionSpec as P

AXES = ("yh", "z", "yl", "x", "core")
ROW = ("z", "yl")
GC = ("yh", "x", "core")
NZ = 32
JUMP = 3
CH = 4
MESH = pl.DeviceIdType.MESH
f32 = jnp.float32
bf16 = jnp.bfloat16

beta_first = 0.9
beta_second = 0.95
learn_rate = 0.002
weight_decay = 0.1
epsilon = 1e-08
first_bias = 1.0 - 0.9**10
second_bias = 1.0 - 0.95**10


def adam_update(gradient, master, moment, second):
    moment_new = beta_first * moment + (1.0 - beta_first) * gradient
    second_new = beta_second * second + (1.0 - beta_second) * gradient * gradient
    direction = moment_new / first_bias / (jnp.sqrt(second_new / second_bias) + epsilon)
    master_new = master - learn_rate * (direction + weight_decay * master)
    return (master_new, moment_new, second_new)


def wrap(v, n):
    return lax.rem(v + 4 * n, n)


def nt(a, b):
    return lax.dot_general(a, b, (((1,), (1,)), ((), ())), preferred_element_type=f32)


def nn(a, b):
    return jnp.dot(a, b, preferred_element_type=f32)


def kernel(
    tok_hbm, cot_hbm, master_hbm, moment_hbm, second_hbm, prompts_hbm, up_hbm, down_hbm,
    master_hout, moment_hout, second_hout, prefill_out,
    master_out, moment_out, second_out,
    tok_ref, cot_ref, master_v, moment_v, second_v, prompts_v, up_v, down_v, dperm, dother,
    tsib, csib, tok_all, cs_send, cot_all, p_all,
    gsend, grecv, rsend, rrecv, rcat,
    gp32, gps, gpr, hid, hrecv, a32, asend, arecv, b32, bsend, brecv,
    loc_sem, st_sem, d2d_s, d2d_r, js, jr, hs, hr, fs, fr,
    c1s, c1r, xs, xr, x2s, x2r, cfs, cfr,
    ps, pr, gs, gr, ds_, dr_, as_, ar, bs, br,
):
    yh, z, yl, x, c = (lax.axis_index(a) for a in AXES)
    h = yh * 4 + x
    zh, zl = z // 4, lax.rem(z, 4)
    sib = {"core": 1 - c}
    yn = {"yl": 1 - yl}
    sends = []

    def remote(src, dst, ssem, rsem, peer):
        return pltpu.make_async_remote_copy(
            src_ref=src, dst_ref=dst, send_sem=ssem, recv_sem=rsem,
            device_id=peer, device_id_type=MESH,
        )

    loads = []
    for n, (a, b) in enumerate(
        ((prompts_hbm, prompts_v), (master_hbm, master_v), (moment_hbm, moment_v),
         (second_hbm, second_v), (down_hbm, down_v), (up_hbm, up_v),
         (tok_hbm, tok_ref), (cot_hbm, cot_ref))
    ):
        cp = pltpu.make_async_copy(a, b, loc_sem.at[n])
        loads.append(cp)
    for n in (6, 7, 0, 4, 1, 2, 3, 5):
        loads[n].start()

    def chip_peer(k):
        o = lax.rem(h + k, 8)
        return o, {"yh": o // 4, "x": lax.rem(o, 4)}

    def prompt_peer(k):
        o = lax.rem(h + k, 8)
        return o, {"yh": o // 4, "x": lax.rem(o, 4), "yl": lax.rem(yl + yh + o // 4, 2)}

    def near_peer(s, k):
        u = wrap(z + 2 * s, NZ)
        to = wrap(u // 4 * 4 + lax.rem(u + k, 4) - 2 * s, NZ)
        return lax.rem(to, 4), {"z": to}

    barrier = pltpu.get_barrier_semaphore()
    peers = [sib, yn]
    peers += [{"z": wrap(z + d, NZ)} for d in (1, -1, JUMP, -JUMP)]
    peers += [near_peer(s, k)[1] for s in range(2) for k in range(1, 4)]
    peers += [chip_peer(k)[1] for k in range(1, 8)]
    peers += [prompt_peer(k)[1] for k in range(1, 8)]
    for peer in peers:
        pl.semaphore_signal(barrier, inc=1, device_id=peer, device_id_type=MESH)
    pl.semaphore_wait(barrier, len(peers))
    loads[6].wait()
    loads[7].wait()

    tok_d2d = remote(tok_ref, tsib, d2d_s.at[0], d2d_r.at[0], sib)
    cot_d2d = remote(cot_ref, csib, d2d_s.at[0], d2d_r.at[0], sib)

    def block(d):
        return wrap(z - d, NZ)

    order = {0: 0}
    for d in range(1, 16):
        order[d] = len(order)
        order[-d] = len(order)
    order[16] = len(order)

    def fwd(d):
        b = tok_all.at[block(d)]
        return remote(b, b, fs.at[order[d]], fr.at[order[d]], sib)

    rows = 64 // CH
    steps = 5

    def side(dr):
        return 0 if dr > 0 else 1

    def piece(d, ch):
        return tok_all.at[block(d), pl.ds(rows * ch, rows)]

    def jump(dr, k, ch):
        b, i = piece(dr * JUMP * k, ch), side(dr)
        return remote(b, b, js.at[i, k], jr.at[i, k, ch], {"z": wrap(z + JUMP * dr, NZ)})

    def jump_in(dr, k, ch):
        b, i = piece(dr * JUMP * (k + 1), ch), side(dr)
        return remote(b, b, js.at[i, k], jr.at[i, k, ch], {"z": wrap(z + JUMP * dr, NZ)})

    def jump_out(dr, k):
        b, i = tok_all.at[block(dr * JUMP * k)], side(dr)
        return remote(b, b, js.at[i, k], jr.at[i, k, 0], {"z": wrap(z + JUMP * dr, NZ)})

    def hop(dr, k, way, ch):
        b, i = piece(dr * JUMP * k, ch), 2 * side(dr) + side(way)
        return remote(b, b, hs.at[i, k], hr.at[i, k], {"z": wrap(z + dr * way, NZ)})

    def hop_out(dr, k, way):
        b, i = tok_all.at[block(dr * JUMP * k)], 2 * side(dr) + side(way)
        return remote(b, b, hs.at[i, k], hr.at[i, k], {"z": wrap(z + dr * way, NZ)})

    def hop_in(dr, k, way):
        b, i = tok_all.at[block(dr * (JUMP * k + way))], 2 * side(dr) + side(way)
        return remote(b, b, hs.at[i, k], hr.at[i, k], {"z": wrap(z + dr * way, NZ)})

    def ways(dr, k):
        return [w for w in (1, -1) if (k > 0 or w > 0) and (dr > 0 or k < steps or w < 0)]

    def prompt_send(k):
        o, peer = prompt_peer(k)
        return remote(
            prompts_v.at[:, pl.ds(pl.multiple_of(o * 640, 128), 640)],
            p_all.at[h], ps.at[k], pr.at[k], peer,
        )

    def send_prompts():
        loads[0].wait()
        for k in range(1, 8):
            prompt_send(k).start()
        p_all[h] = prompts_v[:, pl.ds(pl.multiple_of(h * 640, 128), 640)]

    def hp(j, d):
        return (yh if j < 2 else 1 - yh) * 4 + wrap(x + d, 4)

    def lp(j):
        return yl if j % 2 == 0 else 1 - yl

    def ysend(j):
        src = cs_send if j % 2 else cot_all.at[h, yl]
        peer = {"yh": yh if j < 2 else 1 - yh, "yl": lp(j)}
        return remote(src, cot_all.at[h, yl], c1s.at[j], c1r.at[j], peer)

    def xsend(j, dr):
        b, i = cot_all.at[hp(j, 0), lp(j)], side(dr)
        return remote(b, b, xs.at[i, j], xr.at[i, j], {"x": wrap(x + dr, 4)})

    def x2send(j):
        dr = -1 if j % 2 else 1
        b = cot_all.at[hp(j, -dr), lp(j)]
        return remote(b, b, x2s.at[j], x2r.at[j], {"x": wrap(x + dr, 4)})

    def cfwd(j, d):
        b = cot_all.at[hp(j, d), lp(j)]
        return remote(b, b, cfs.at[j, d], cfr.at[j, d], sib)

    down_y = remote(dperm.at[1 - yl], dother, ds_.at[0], dr_.at[0], yn)
    down_own = remote(dperm.at[yl], dperm.at[yl], ds_.at[1], dr_.at[1], sib)
    down_sib = remote(dother, dother, ds_.at[2], dr_.at[2], sib)

    def arrange(l):
        for zz in range(32):
            col = 80 * (2 * zz + l)
            at, part = zz % 4 * 640, zz // 4
            dperm[l, :, at + 64 * part : at + 64 * part + 64] = down_v[:, col : col + 64]
            at += 512 + 16 * part
            dperm[l, :, at : at + 16] = down_v[:, col + 64 : col + 80]

    @pl.when(c == 1)
    def _():
        cot_d2d.start()
        tok_d2d.wait_recv()
        mine, other = tok_ref[...], tsib[...]
        tok_all[z] = jnp.concatenate(
            [other[:, :256], mine[:, :256], other[:, 256:], mine[:, 256:]], axis=1
        )
        for ch in range(CH):
            for dr in (1, -1):
                jump(dr, 0, ch).start()
            for dr in (1, -1):
                hop(dr, 0, 1, ch).start()
        fwd(0).start()
        for k in range(1, steps + 1):
            for ch in range(CH):
                for dr in (1, -1):
                    jump_in(dr, k - 1, ch).wait_recv()
                    if k < steps:
                        jump(dr, k, ch).start()
                    for way in ways(dr, k):
                        hop(dr, k, way, ch).start()
                    if ch == CH - 1:
                        fwd(dr * JUMP * k).start()
            if k == 2:
                send_prompts()
            for dr in (1, -1):
                for way in ways(dr, k - 1):
                    hop_in(dr, k - 1, way).wait_recv()
                    fwd(dr * (JUMP * (k - 1) + way)).start()
        for dr in (1, -1):
            for way in ways(dr, steps):
                hop_in(dr, steps, way).wait_recv()
                fwd(dr * (JUMP * steps + way)).start()
        for j in range(4):
            for d in range(4):
                cfwd(j, d).wait_recv()

    @pl.when(c == 0)
    def _():
        tok_d2d.start()
        cot_d2d.wait_recv()
        for core, src in ((0, cot_ref), (1, csib)):
            v = src[...]
            even = jnp.concatenate([v[:, :64], v[:, 128:192]], axis=1)
            odd = jnp.concatenate([v[:, 64:128], v[:, 192:]], axis=1)
            first = yl == 0
            cot_all[h, yl, core] = jnp.where(first, even, odd)
            cs_send[core] = jnp.where(first, odd, even)
        for j in (1, 3, 2):
            ysend(j).start()
        for j in (0, 1, 3, 2):
            if j:
                ysend(j).wait_recv()
            for dr in (1, -1):
                xsend(j, dr).start()
            cfwd(j, 0).start()
        loads[4].wait()
        for l in range(2):
            @pl.when(yl != l)
            def _():
                arrange(l)
        down_y.start()
        for j in (0, 1, 3, 2):
            for dr in (1, -1):
                xsend(j, dr).wait_recv()
                if dr == (-1 if j % 2 else 1):
                    x2send(j).start()
                cfwd(j, 1 if dr < 0 else 3).start()
        send_prompts()
        for j in (0, 1, 3, 2):
            x2send(j).wait_recv()
            cfwd(j, 2).start()
        for l in range(2):
            @pl.when(yl == l)
            def _():
                arrange(l)
        down_own.start()
        for d in order:
            fwd(d).wait_recv()

    first_core = c == 0

    def gradient(part):
        wide = jnp.zeros((200, 256), f32)
        rest = jnp.zeros((200, 128), f32)
        for o in range(8):
            lhs = jnp.concatenate([cot_all[o, part, 0], cot_all[o, part, 1]], axis=1)
            t = tok_all[4 * o : 4 * o + 4, :, pl.ds(pl.multiple_of(c * 256, 256), 256)]
            wide += nn(lhs, t.reshape(256, 256))
            rest += nn(lhs, tok_all[4 * o : 4 * o + 4, :, 512:640].reshape(256, 128))
        return wide, jnp.where(first_core, rest[:, :64], rest[:, 64:])

    wide, rest = gradient(1 - yl)
    gsend[:, :256] = wide.astype(bf16)
    gsend[:, 256:] = rest.astype(bf16)
    gcp = remote(gsend, grecv, d2d_s.at[1], d2d_r.at[1], yn)
    gcp.start()
    wide, rest = gradient(yl)
    for n in (1, 2, 3):
        loads[n].wait()
    gcp.wait_recv()
    for part, lanes in ((wide, slice(0, 256)), (rest, slice(256, 320))):
        total = part + grecv[:, lanes].astype(f32)
        new = adam_update(total, master_v[:, lanes], moment_v[:, lanes], second_v[:, lanes])
        master_out[:, lanes] = new[0]
        moment_out[:, lanes] = new[1]
        second_out[:, lanes] = new[2]
        rsend[:, lanes] = new[0].astype(bf16)
    stores = []
    for n, (a, b) in enumerate(
        ((master_out, master_hout), (moment_out, moment_hout), (second_out, second_hout))
    ):
        stores.append(pltpu.make_async_copy(a, b, st_sem.at[n]))
    rcp = remote(rsend, rrecv, d2d_s.at[2], d2d_r.at[2], sib)
    rcp.start()
    for cp in stores:
        cp.start()

    @pl.when(c == 0)
    def _():
        down_y.wait_recv()
        down_sib.start()

    for k in range(1, 8):
        prompt_send(k).wait_recv()
    rcp.wait_recv()
    mine, other = rsend[...], rrecv[...]
    rcat[:, :320] = jnp.where(first_core, mine, other)
    rcat[:, 320:] = jnp.where(first_core, other, mine)

    for o in range(8):
        v = nt(p_all[o], rcat[...])
        gp32[o] = v
        gps[o] = v.astype(bf16)

    def gate_send(k):
        o, peer = chip_peer(k)
        return remote(gps.at[o], gpr.at[h], gs.at[k], gr.at[k], peer)

    for k in (4, 2, 6, 1, 3, 5, 7):
        gate_send(k).start()
    loads[5].wait()
    up_pre = nt(prompts_v[...], up_v[...])
    gate = gp32[h]
    for k in range(1, 8):
        gate_send(k).wait_recv()
        gate += gpr[wrap(h - k, 8)].astype(f32)
    hidden = (gate / (1.0 + jnp.exp(-gate)) * up_pre).astype(bf16)
    hid[...] = hidden
    hcp = remote(hid, hrecv, d2d_s.at[3], d2d_r.at[3], yn)
    hcp.start()

    @pl.when(c == 1)
    def _():
        down_own.wait_recv()
        down_sib.wait_recv()

    for o in range(4):
        a32[o] = nn(hidden, dperm[yl, :, 640 * o : 640 * o + 640])
    hcp.wait_recv()
    hidden = hrecv[...]

    def near_send(s, k):
        o, peer = near_peer(s, k)
        part = pl.ds(32 * s, 32)
        return remote(asend.at[o, part], arecv.at[k - 1, part], as_.at[s, k], ar.at[s, k], peer)

    for o in range(4):
        v = a32[o] + nn(hidden, dother[:, 640 * o : 640 * o + 640])
        a32[o] = v
        asend[o] = v.astype(bf16)
    for s in range(2):
        for k in (2, 1, 3):
            near_send(s, k).start()

    def far_send(k):
        o = lax.rem(zh + k, 8)
        return remote(bsend.at[o], brecv.at[k - 1], bs.at[k], br.at[k], {"z": o * 4 + zl})

    for s in range(2):
        part = slice(32 * s, 32 * s + 32)
        total = a32[zl, part]
        for k in range(1, 4):
            near_send(s, k).wait_recv()
            total += arecv[k - 1, part].astype(f32)
        a32[zl, part] = total
    lane = lax.broadcasted_iota(jnp.int32, (32, 128), 1)
    for o in range(4):
        top = a32[zl, :32, 128 * o : 128 * o + 128]
        low = a32[zl, 32:, 128 * o : 128 * o + 128]
        even = jnp.where(lane < 64, top, pltpu.roll(low, 64, 1))
        odd = jnp.where(lane < 64, pltpu.roll(top, 64, 1), low)
        b32[2 * o, :32], b32[2 * o + 1, :32] = even, odd
        bsend[2 * o, :32], bsend[2 * o + 1, :32] = even.astype(bf16), odd.astype(bf16)
    last = a32[zl, :, 512:640]
    rolled = [last] + [pltpu.roll(last, 16 * n, 1) for n in range(1, 8)]
    sixteen = lax.broadcasted_iota(jnp.int32, (8, 128), 1) // 16
    for o in range(8):
        v = rolled[-o % 8][:8]
        for q in range(1, 8):
            v = jnp.where(sixteen == q, rolled[(q - o) % 8][8 * q : 8 * q + 8], v)
        b32[o, 32:] = v
        bsend[o, 32:] = v.astype(bf16)
    for k in (4, 3, 5, 2, 6, 1, 7):
        far_send(k).start()
    total = b32[zh]
    for k in (1, 7, 2, 6, 3, 5, 4):
        far_send(k).wait_recv()
        total += brecv[k - 1].astype(f32)
    prefill_out[:32, :64] = total[:32, :64]
    prefill_out[32:, :64] = total[:32, 64:]
    for q in range(8):
        prefill_out[8 * q : 8 * q + 8, 64:] = total[32:, 16 * q : 16 * q + 16]

    @pl.when(c == 1)
    def _():
        cot_d2d.wait_send()
        for dr in (1, -1):
            for k in range(steps + 1):
                if k < steps:
                    jump_out(dr, k).wait_send()
                for way in ways(dr, k):
                    hop_out(dr, k, way).wait_send()
        for d in order:
            fwd(d).wait_send()

    @pl.when(c == 0)
    def _():
        tok_d2d.wait_send()
        down_y.wait_send()
        down_own.wait_send()
        down_sib.wait_send()
        for j in range(4):
            if j:
                ysend(j).wait_send()
            for dr in (1, -1):
                xsend(j, dr).wait_send()
            x2send(j).wait_send()
            for d in range(4):
                cfwd(j, d).wait_send()

    @pl.when(c == 1)
    def _():
        loads[4].wait()

    for cp in stores:
        cp.wait()
    for cp in (gcp, rcp, hcp):
        cp.wait_send()
    for k in range(1, 8):
        prompt_send(k).wait_send()
        gate_send(k).wait_send()
        far_send(k).wait_send()
    for s in range(2):
        for k in range(1, 4):
            near_send(s, k).wait_send()


def deliver(*refs):
    ins, outs, held, (in_sem, out_sem) = refs[:4], refs[4:8], refs[8:12], refs[12:]
    reads = [pltpu.make_async_copy(ins[n], held[n], in_sem.at[n]) for n in range(4)]
    writes = [pltpu.make_async_copy(held[n], outs[n], out_sem.at[n]) for n in range(4)]
    for cp in reads:
        cp.start()
    for n in range(4):
        reads[n].wait()
        writes[n].start()
    for cp in writes:
        cp.wait()


def shards(tokens, cotangent, master, moment, second, prompts, up_weight, down_weight):
    V, D = pltpu.VMEM, pltpu.SemaphoreType.DMA
    vmem = pl.BlockSpec(memory_space=pltpu.VMEM)
    hbm = pl.BlockSpec(memory_space=pltpu.HBM)
    out = jax.ShapeDtypeStruct
    results = pl.pallas_call(
        kernel,
        out_shape=(
            out((200, 320), f32), out((200, 320), f32), out((200, 320), f32), out((64, 80), f32),
        ),
        in_specs=[hbm] * 8,
        out_specs=[hbm] * 3 + [vmem],
        scratch_shapes=[
            V((200, 320), f32), V((200, 320), f32), V((200, 320), f32),
            V((64, 320), bf16), V((200, 256), bf16),
            V((200, 320), f32), V((200, 320), f32), V((200, 320), f32),
            V((64, 5120), bf16), V((200, 5120), bf16), V((200, 5120), bf16),
            V((2, 200, 2560), bf16), V((200, 2560), bf16),
            V((64, 320), bf16), V((200, 256), bf16), V((32, 64, 640), bf16),
            V((2, 200, 128), bf16), V((8, 2, 2, 200, 128), bf16), V((8, 64, 640), bf16),
            V((200, 320), bf16), V((200, 320), bf16), V((200, 320), bf16), V((200, 320), bf16),
            V((200, 640), bf16),
            V((8, 64, 200), f32), V((8, 64, 200), bf16), V((8, 64, 200), bf16),
            V((64, 200), bf16), V((64, 200), bf16),
            V((4, 64, 640), f32), V((4, 64, 640), bf16), V((3, 64, 640), bf16),
            V((8, 40, 128), f32), V((8, 40, 128), bf16), V((7, 40, 128), bf16),
            D((8,)), D((3,)), D((4,)), D((4,)), D((2, 5)), D((2, 5, CH)), D((4, 6)), D((4, 6)),
            D((32,)), D((32,)),
            D((4,)), D((4,)), D((2, 4)), D((2, 4)), D((4,)), D((4,)),
            D((4, 4)), D((4, 4)),
            D((8,)), D((8,)), D((8,)), D((8,)), D((3,)), D((3,)),
            D((2, 4)), D((2, 4)), D((8,)), D((8,)),
        ],
        compiler_params=pltpu.CompilerParams(
            collective_id=0, has_side_effects=True, vmem_limit_bytes=65_900_000
        ),
    )(tokens, cotangent.T, master, moment, second, prompts, up_weight, down_weight)
    return pl.pallas_call(
        deliver,
        out_shape=tuple(out(r.shape, f32) for r in results),
        in_specs=[hbm] * 4,
        out_specs=[hbm] * 4,
        scratch_shapes=[V(r.shape, f32) for r in results] + [D((4,)), D((4,))],
        compiler_params=pltpu.CompilerParams(vmem_limit_bytes=65_900_000),
    )(*results)


def solution(mesh):
    split = Mesh(mesh.devices.reshape(2, NZ, 2, 4, 2), AXES)
    tile, rows = P(ROW, GC), P(GC, ROW)
    return jax.shard_map(
        shards,
        mesh=split,
        in_specs=(tile, rows, tile, tile, tile, P(GC, None), P(ROW, None), P(ROW, None)),
        out_specs=(tile, tile, tile, rows),
        check_vma=False,
    )
```

```python
import functools

import jax
import jax.numpy as jnp
from jax import lax
from jax.experimental import pallas as pl
from jax.experimental.pallas import tpu as pltpu
from jax.sharding import Mesh
from jax.sharding import PartitionSpec as P

AXES = ("yh", "z", "yl", "x", "core")
ROW = ("z", "yl")
GC = ("yh", "x", "core")
NZ = 32
JUMP = 3
CH = 4
MESH = pl.DeviceIdType.MESH
f32 = jnp.float32
bf16 = jnp.bfloat16

beta_first = 0.9
beta_second = 0.95
learn_rate = 0.002
weight_decay = 0.1
epsilon = 1e-08
first_bias = 1.0 - 0.9**10
second_bias = 1.0 - 0.95**10


def adam_update(gradient, master, moment, second):
    moment_new = beta_first * moment + (1.0 - beta_first) * gradient
    second_new = beta_second * second + (1.0 - beta_second) * gradient * gradient
    direction = moment_new / first_bias / (jnp.sqrt(second_new / second_bias) + epsilon)
    master_new = master - learn_rate * (direction + weight_decay * master)
    return (master_new, moment_new, second_new)


def wrap(v, n):
    return lax.rem(v + 4 * n, n)


def nt(a, b):
    return lax.dot_general(a, b, (((1,), (1,)), ((), ())), preferred_element_type=f32)


def nn(a, b):
    return jnp.dot(a, b, preferred_element_type=f32)


def kernel(
    tok_hbm, cot_hbm, master_hbm, moment_hbm, second_hbm, prompts_hbm, up_hbm, down_hbm,
    master_hout, moment_hout, second_hout, prefill_out,
    master_out, moment_out, second_out,
    tok_ref, cot_ref, master_v, moment_v, second_v, prompts_v, up_v, down_v, dperm, dother,
    tsib, csib, tok_all, cs_send, cot_all, p_all,
    gsend, grecv, rsend, rrecv, rcat,
    gp32, gps, gpr, hid, hrecv, a32, asend, arecv, b32, bsend, brecv,
    loc_sem, st_sem, d2d_s, d2d_r, js, jr, hs, hr, fs, fr,
    c1s, c1r, xs, xr, x2s, x2r, cfs, cfr,
    ps, pr, gs, gr, ds_, dr_, as_, ar, bs, br,
):
    yh, z, yl, x, c = (lax.axis_index(a) for a in AXES)
    h = yh * 4 + x
    zh, zl = z // 4, lax.rem(z, 4)
    sib = {"core": 1 - c}
    yn = {"yl": 1 - yl}
    sends = []

    def remote(src, dst, ssem, rsem, peer):
        return pltpu.make_async_remote_copy(
            src_ref=src, dst_ref=dst, send_sem=ssem, recv_sem=rsem,
            device_id=peer, device_id_type=MESH,
        )

    loads = []
    for n, (a, b) in enumerate(
        ((prompts_hbm, prompts_v), (master_hbm, master_v), (moment_hbm, moment_v),
         (second_hbm, second_v), (down_hbm, down_v), (up_hbm, up_v),
         (tok_hbm, tok_ref), (cot_hbm, cot_ref))
    ):
        cp = pltpu.make_async_copy(a, b, loc_sem.at[n])
        loads.append(cp)
    for n in (6, 7, 0, 4, 1, 2, 3, 5):
        loads[n].start()

    def chip_peer(k):
        o = lax.rem(h + k, 8)
        return o, {"yh": o // 4, "x": lax.rem(o, 4)}

    def prompt_peer(k):
        o = lax.rem(h + k, 8)
        return o, {"yh": o // 4, "x": lax.rem(o, 4), "yl": lax.rem(yl + yh + o // 4, 2)}

    def near_peer(s, k):
        u = wrap(z + 2 * s, NZ)
        to = wrap(u // 4 * 4 + lax.rem(u + k, 4) - 2 * s, NZ)
        return lax.rem(to, 4), {"z": to}

    barrier = pltpu.get_barrier_semaphore()
    peers = [sib, yn]
    peers += [{"z": wrap(z + d, NZ)} for d in (1, -1, JUMP, -JUMP)]
    peers += [near_peer(s, k)[1] for s in range(2) for k in range(1, 4)]
    peers += [chip_peer(k)[1] for k in range(1, 8)]
    peers += [prompt_peer(k)[1] for k in range(1, 8)]
    for peer in peers:
        pl.semaphore_signal(barrier, inc=1, device_id=peer, device_id_type=MESH)
    pl.semaphore_wait(barrier, len(peers))
    loads[6].wait()
    loads[7].wait()

    tok_d2d = remote(tok_ref, tsib, d2d_s.at[0], d2d_r.at[0], sib)
    cot_d2d = remote(cot_ref, csib, d2d_s.at[0], d2d_r.at[0], sib)

    def block(d):
        return wrap(z - d, NZ)

    order = {0: 0}
    for d in range(1, 16):
        order[d] = len(order)
        order[-d] = len(order)
    order[16] = len(order)

    def fwd(d):
        b = tok_all.at[block(d)]
        return remote(b, b, fs.at[order[d]], fr.at[order[d]], sib)

    rows = 64 // CH
    steps = 5

    def side(dr):
        return 0 if dr > 0 else 1

    def piece(d, ch):
        return tok_all.at[block(d), pl.ds(rows * ch, rows)]

    def jump(dr, k, ch):
        b, i = piece(dr * JUMP * k, ch), side(dr)
        return remote(b, b, js.at[i, k], jr.at[i, k, ch], {"z": wrap(z + JUMP * dr, NZ)})

    def jump_in(dr, k, ch):
        b, i = piece(dr * JUMP * (k + 1), ch), side(dr)
        return remote(b, b, js.at[i, k], jr.at[i, k, ch], {"z": wrap(z + JUMP * dr, NZ)})

    def jump_out(dr, k):
        b, i = tok_all.at[block(dr * JUMP * k)], side(dr)
        return remote(b, b, js.at[i, k], jr.at[i, k, 0], {"z": wrap(z + JUMP * dr, NZ)})

    def hop(dr, k, way, ch):
        b, i = piece(dr * JUMP * k, ch), 2 * side(dr) + side(way)
        return remote(b, b, hs.at[i, k], hr.at[i, k], {"z": wrap(z + dr * way, NZ)})

    def hop_out(dr, k, way):
        b, i = tok_all.at[block(dr * JUMP * k)], 2 * side(dr) + side(way)
        return remote(b, b, hs.at[i, k], hr.at[i, k], {"z": wrap(z + dr * way, NZ)})

    def hop_in(dr, k, way):
        b, i = tok_all.at[block(dr * (JUMP * k + way))], 2 * side(dr) + side(way)
        return remote(b, b, hs.at[i, k], hr.at[i, k], {"z": wrap(z + dr * way, NZ)})

    def ways(dr, k):
        return [w for w in (1, -1) if (k > 0 or w > 0) and (dr > 0 or k < steps or w < 0)]

    def prompt_send(k):
        o, peer = prompt_peer(k)
        return remote(
            prompts_v.at[:, pl.ds(pl.multiple_of(o * 640, 128), 640)],
            p_all.at[h], ps.at[k], pr.at[k], peer,
        )

    def send_prompts():
        loads[0].wait()
        for k in range(1, 8):
            prompt_send(k).start()
        p_all[h] = prompts_v[:, pl.ds(pl.multiple_of(h * 640, 128), 640)]

    def hp(j, d):
        return (yh if j < 2 else 1 - yh) * 4 + wrap(x + d, 4)

    def lp(j):
        return yl if j % 2 == 0 else 1 - yl

    def ysend(j):
        src = cs_send if j % 2 else cot_all.at[h, yl]
        peer = {"yh": yh if j < 2 else 1 - yh, "yl": lp(j)}
        return remote(src, cot_all.at[h, yl], c1s.at[j], c1r.at[j], peer)

    def xsend(j, dr):
        b, i = cot_all.at[hp(j, 0), lp(j)], side(dr)
        return remote(b, b, xs.at[i, j], xr.at[i, j], {"x": wrap(x + dr, 4)})

    def x2send(j):
        dr = -1 if j % 2 else 1
        b = cot_all.at[hp(j, -dr), lp(j)]
        return remote(b, b, x2s.at[j], x2r.at[j], {"x": wrap(x + dr, 4)})

    def cfwd(j, d):
        b = cot_all.at[hp(j, d), lp(j)]
        return remote(b, b, cfs.at[j, d], cfr.at[j, d], sib)

    down_y = remote(dperm.at[1 - yl], dother, ds_.at[0], dr_.at[0], yn)
    down_own = remote(dperm.at[yl], dperm.at[yl], ds_.at[1], dr_.at[1], sib)
    down_sib = remote(dother, dother, ds_.at[2], dr_.at[2], sib)

    def arrange(l):
        for zz in range(32):
            col = 80 * (2 * zz + l)
            at, part = zz % 4 * 640, zz // 4
            dperm[l, :, at + 64 * part : at + 64 * part + 64] = down_v[:, col : col + 64]
            at += 512 + 16 * part
            dperm[l, :, at : at + 16] = down_v[:, col + 64 : col + 80]

    @pl.when(c == 1)
    def _():
        cot_d2d.start()
        tok_d2d.wait_recv()
        mine, other = tok_ref[...], tsib[...]
        tok_all[z] = jnp.concatenate(
            [other[:, :256], mine[:, :256], other[:, 256:], mine[:, 256:]], axis=1
        )
        for ch in range(CH):
            for dr in (1, -1):
                jump(dr, 0, ch).start()
            for dr in (1, -1):
                hop(dr, 0, 1, ch).start()
        fwd(0).start()
        for k in range(1, steps + 1):
            for ch in range(CH):
                for dr in (1, -1):
                    jump_in(dr, k - 1, ch).wait_recv()
                    if k < steps:
                        jump(dr, k, ch).start()
                    for way in ways(dr, k):
                        hop(dr, k, way, ch).start()
                    if ch == CH - 1:
                        fwd(dr * JUMP * k).start()
            if k == 4:
                send_prompts()
            for dr in (1, -1):
                for way in ways(dr, k - 1):
                    hop_in(dr, k - 1, way).wait_recv()
                    fwd(dr * (JUMP * (k - 1) + way)).start()
        for dr in (1, -1):
            for way in ways(dr, steps):
                hop_in(dr, steps, way).wait_recv()
                fwd(dr * (JUMP * steps + way)).start()
        for j in range(4):
            for d in range(4):
                cfwd(j, d).wait_recv()

    @pl.when(c == 0)
    def _():
        tok_d2d.start()
        cot_d2d.wait_recv()
        for core, src in ((0, cot_ref), (1, csib)):
            v = src[...]
            even = jnp.concatenate([v[:, :64], v[:, 128:192]], axis=1)
            odd = jnp.concatenate([v[:, 64:128], v[:, 192:]], axis=1)
            first = yl == 0
            cot_all[h, yl, core] = jnp.where(first, even, odd)
            cs_send[core] = jnp.where(first, odd, even)
        for j in (1, 3, 2):
            ysend(j).start()
        for j in (0, 1, 3, 2):
            if j:
                ysend(j).wait_recv()
            for dr in (1, -1):
                xsend(j, dr).start()
            cfwd(j, 0).start()
        for j in (0, 1, 3, 2):
            for dr in (1, -1):
                xsend(j, dr).wait_recv()
                if dr == (-1 if j % 2 else 1):
                    x2send(j).start()
                cfwd(j, 1 if dr < 0 else 3).start()
        loads[4].wait()
        for l in range(2):
            @pl.when(yl != l)
            def _():
                arrange(l)
        down_y.start()
        send_prompts()
        for j in (0, 1, 3, 2):
            x2send(j).wait_recv()
            cfwd(j, 2).start()
        for l in range(2):
            @pl.when(yl == l)
            def _():
                arrange(l)
        down_own.start()
        for d in order:
            fwd(d).wait_recv()

    first_core = c == 0

    def gradient(part):
        wide = jnp.zeros((200, 256), f32)
        rest = jnp.zeros((200, 128), f32)
        for o in range(8):
            lhs = jnp.concatenate([cot_all[o, part, 0], cot_all[o, part, 1]], axis=1)
            t = tok_all[4 * o : 4 * o + 4, :, pl.ds(pl.multiple_of(c * 256, 256), 256)]
            wide += nn(lhs, t.reshape(256, 256))
            rest += nn(lhs, tok_all[4 * o : 4 * o + 4, :, 512:640].reshape(256, 128))
        return wide, jnp.where(first_core, rest[:, :64], rest[:, 64:])

    wide, rest = gradient(1 - yl)
    gsend[:, :256] = wide.astype(bf16)
    gsend[:, 256:] = rest.astype(bf16)
    gcp = remote(gsend, grecv, d2d_s.at[1], d2d_r.at[1], yn)
    gcp.start()
    wide, rest = gradient(yl)
    for n in (1, 2, 3):
        loads[n].wait()
    gcp.wait_recv()
    for part, lanes in ((wide, slice(0, 256)), (rest, slice(256, 320))):
        total = part + grecv[:, lanes].astype(f32)
        new = adam_update(total, master_v[:, lanes], moment_v[:, lanes], second_v[:, lanes])
        master_out[:, lanes] = new[0]
        moment_out[:, lanes] = new[1]
        second_out[:, lanes] = new[2]
        rsend[:, lanes] = new[0].astype(bf16)
    stores = []
    for n, (a, b) in enumerate(
        ((master_out, master_hout), (moment_out, moment_hout), (second_out, second_hout))
    ):
        stores.append(pltpu.make_async_copy(a, b, st_sem.at[n]))
    rcp = remote(rsend, rrecv, d2d_s.at[2], d2d_r.at[2], sib)
    rcp.start()
    for cp in stores:
        cp.start()

    @pl.when(c == 0)
    def _():
        down_y.wait_recv()
        down_sib.start()

    for k in range(1, 8):
        prompt_send(k).wait_recv()
    rcp.wait_recv()
    mine, other = rsend[...], rrecv[...]
    rcat[:, :320] = jnp.where(first_core, mine, other)
    rcat[:, 320:] = jnp.where(first_core, other, mine)

    v = nt(p_all[...].reshape(512, 640), rcat[...]).reshape(8, 64, 200)
    gps[...] = v.astype(bf16)
    gp32[...] = v

    def gate_send(k):
        o, peer = chip_peer(k)
        return remote(gps.at[o], gpr.at[h], gs.at[k], gr.at[k], peer)

    for k in (4, 2, 6, 1, 3, 5, 7):
        gate_send(k).start()
    loads[5].wait()
    up_pre = nt(prompts_v[...], up_v[...])
    gate = gp32[h]
    for k in range(1, 8):
        gate_send(k).wait_recv()
        gate += gpr[wrap(h - k, 8)].astype(f32)
    hidden = (gate / (1.0 + jnp.exp(-gate)) * up_pre).astype(bf16)
    hid[...] = hidden
    hcp = remote(hid, hrecv, d2d_s.at[3], d2d_r.at[3], yn)
    hcp.start()

    @pl.when(c == 1)
    def _():
        down_own.wait_recv()
        down_sib.wait_recv()

    for o in range(4):
        a32[o] = nn(hidden, dperm[yl, :, 640 * o : 640 * o + 640])
    hcp.wait_recv()
    hidden = hrecv[...]

    def near_send(s, k):
        o, peer = near_peer(s, k)
        part = pl.ds(32 * s, 32)
        return remote(asend.at[o, part], arecv.at[k - 1, part], as_.at[s, k], ar.at[s, k], peer)

    for k in (2, 1, 3, 0):
        o = lax.rem(zl + k, 4)
        v = a32[o] + nn(hidden, dother[:, pl.ds(pl.multiple_of(640 * o, 128), 640)])
        if k == 0:
            a32[o] = v
        else:
            asend[o] = v.astype(bf16)
            for s in range(2):
                near_send(s, k).start()

    def far_send(k):
        o = lax.rem(zh + k, 8)
        return remote(bsend.at[o], brecv.at[k - 1], bs.at[k], br.at[k], {"z": o * 4 + zl})

    for s in range(2):
        part = slice(32 * s, 32 * s + 32)
        total = a32[zl, part]
        for k in range(1, 4):
            near_send(s, k).wait_recv()
            total += arecv[k - 1, part].astype(f32)
        a32[zl, part] = total
    lane = lax.broadcasted_iota(jnp.int32, (32, 128), 1)
    for o in range(4):
        top = a32[zl, :32, 128 * o : 128 * o + 128]
        low = a32[zl, 32:, 128 * o : 128 * o + 128]
        even = jnp.where(lane < 64, top, pltpu.roll(low, 64, 1))
        odd = jnp.where(lane < 64, pltpu.roll(top, 64, 1), low)
        b32[2 * o, :32], b32[2 * o + 1, :32] = even, odd
        bsend[2 * o, :32], bsend[2 * o + 1, :32] = even.astype(bf16), odd.astype(bf16)
    last = a32[zl, :, 512:640]
    rolled = [last] + [pltpu.roll(last, 16 * n, 1) for n in range(1, 8)]
    sixteen = lax.broadcasted_iota(jnp.int32, (8, 128), 1) // 16
    for o in range(8):
        v = rolled[-o % 8][:8]
        for q in range(1, 8):
            v = jnp.where(sixteen == q, rolled[(q - o) % 8][8 * q : 8 * q + 8], v)
        b32[o, 32:] = v
        bsend[o, 32:] = v.astype(bf16)
    for k in (4, 3, 5, 2, 6, 1, 7):
        far_send(k).start()
    total = b32[zh]
    for k in (1, 7, 2, 6, 3, 5, 4):
        far_send(k).wait_recv()
        total += brecv[k - 1].astype(f32)
    prefill_out[:32, :64] = total[:32, :64]
    prefill_out[32:, :64] = total[:32, 64:]
    for q in range(8):
        prefill_out[8 * q : 8 * q + 8, 64:] = total[32:, 16 * q : 16 * q + 16]

    @pl.when(c == 1)
    def _():
        cot_d2d.wait_send()
        for dr in (1, -1):
            for k in range(steps + 1):
                if k < steps:
                    jump_out(dr, k).wait_send()
                for way in ways(dr, k):
                    hop_out(dr, k, way).wait_send()
        for d in order:
            fwd(d).wait_send()

    @pl.when(c == 0)
    def _():
        tok_d2d.wait_send()
        down_y.wait_send()
        down_own.wait_send()
        down_sib.wait_send()
        for j in range(4):
            if j:
                ysend(j).wait_send()
            for dr in (1, -1):
                xsend(j, dr).wait_send()
            x2send(j).wait_send()
            for d in range(4):
                cfwd(j, d).wait_send()

    @pl.when(c == 1)
    def _():
        loads[4].wait()

    for cp in stores:
        cp.wait()
    for cp in (gcp, rcp, hcp):
        cp.wait_send()
    for k in range(1, 8):
        prompt_send(k).wait_send()
        gate_send(k).wait_send()
        far_send(k).wait_send()
    for s in range(2):
        for k in range(1, 4):
            near_send(s, k).wait_send()


def deliver(*refs):
    ins, outs, held, (in_sem, out_sem) = refs[:4], refs[4:8], refs[8:12], refs[12:]
    reads = [pltpu.make_async_copy(ins[n], held[n], in_sem.at[n]) for n in range(4)]
    writes = [pltpu.make_async_copy(held[n], outs[n], out_sem.at[n]) for n in range(4)]
    for cp in reads:
        cp.start()
    for n in range(4):
        reads[n].wait()
        writes[n].start()
    for cp in writes:
        cp.wait()


def shards(tokens, cotangent, master, moment, second, prompts, up_weight, down_weight):
    V, D = pltpu.VMEM, pltpu.SemaphoreType.DMA
    vmem = pl.BlockSpec(memory_space=pltpu.VMEM)
    hbm = pl.BlockSpec(memory_space=pltpu.HBM)
    out = jax.ShapeDtypeStruct
    results = pl.pallas_call(
        kernel,
        out_shape=(
            out((200, 320), f32), out((200, 320), f32), out((200, 320), f32), out((64, 80), f32),
        ),
        in_specs=[hbm] * 8,
        out_specs=[hbm] * 3 + [vmem],
        scratch_shapes=[
            V((200, 320), f32), V((200, 320), f32), V((200, 320), f32),
            V((64, 320), bf16), V((200, 256), bf16),
            V((200, 320), f32), V((200, 320), f32), V((200, 320), f32),
            V((64, 5120), bf16), V((200, 5120), bf16), V((200, 5120), bf16),
            V((2, 200, 2560), bf16), V((200, 2560), bf16),
            V((64, 320), bf16), V((200, 256), bf16), V((32, 64, 640), bf16),
            V((2, 200, 128), bf16), V((8, 2, 2, 200, 128), bf16), V((8, 64, 640), bf16),
            V((200, 320), bf16), V((200, 320), bf16), V((200, 320), bf16), V((200, 320), bf16),
            V((200, 640), bf16),
            V((8, 64, 200), f32), V((8, 64, 200), bf16), V((8, 64, 200), bf16),
            V((64, 200), bf16), V((64, 200), bf16),
            V((4, 64, 640), f32), V((4, 64, 640), bf16), V((3, 64, 640), bf16),
            V((8, 40, 128), f32), V((8, 40, 128), bf16), V((7, 40, 128), bf16),
            D((8,)), D((3,)), D((4,)), D((4,)), D((2, 5)), D((2, 5, CH)), D((4, 6)), D((4, 6)),
            D((32,)), D((32,)),
            D((4,)), D((4,)), D((2, 4)), D((2, 4)), D((4,)), D((4,)),
            D((4, 4)), D((4, 4)),
            D((8,)), D((8,)), D((8,)), D((8,)), D((3,)), D((3,)),
            D((2, 4)), D((2, 4)), D((8,)), D((8,)),
        ],
        compiler_params=pltpu.CompilerParams(
            collective_id=0, has_side_effects=True, vmem_limit_bytes=65_900_000
        ),
    )(tokens, cotangent.T, master, moment, second, prompts, up_weight, down_weight)
    return pl.pallas_call(
        deliver,
        out_shape=tuple(out(r.shape, f32) for r in results),
        in_specs=[hbm] * 4,
        out_specs=[hbm] * 4,
        scratch_shapes=[V(r.shape, f32) for r in results] + [D((4,)), D((4,))],
        compiler_params=pltpu.CompilerParams(vmem_limit_bytes=65_900_000),
    )(*results)


def solution(mesh):
    split = Mesh(mesh.devices.reshape(2, NZ, 2, 4, 2), AXES)
    tile, rows = P(ROW, GC), P(GC, ROW)
    return jax.shard_map(
        shards,
        mesh=split,
        in_specs=(tile, rows, tile, tile, tile, P(GC, None), P(ROW, None), P(ROW, None)),
        out_specs=(tile, tile, tile, rows),
        check_vma=False,
    )
```
